32 devices in a mesh: tp: 4 (over z), fsdp: 8 (over y, x, core).
Axes of the slice: x: 2, y: 2, z: 4, core: 2. Of those that a mesh axis runs over, the one named last changes fastest.
Arguments:
- x_in: bfloat16 [16, 1024, 2048], P('fsdp')
- ln_gain: float32 [2048], replicated
- w_q: bfloat16 [2048, 2048], P('fsdp', 'tp')
- w_kv: bfloat16 [2048, 512], P('fsdp')
- w_gu: bfloat16 [2048, 2, 8192], P('fsdp', None, 'tp')
- w_oa: bfloat16 [2048, 2048], P('tp', 'fsdp')
- w_om: bfloat16 [8192, 2048], P('tp', 'fsdp')
- dy_in: bfloat16 [16, 1024, 2048], P('fsdp')
Outputs:
- output 1: bfloat16 [16, 1024, 2048], P('fsdp')
- output 2: bfloat16 [16, 1024, 2048], P('fsdp')
- output 3: float32 [2048], replicated
- output 4: bfloat16 [2048, 2048], P('fsdp', 'tp')
- output 5: bfloat16 [2048, 512], P('fsdp')
- output 6: bfloat16 [2048, 2, 8192], P('fsdp', None, 'tp')
- output 7: bfloat16 [2048, 2048], P('tp', 'fsdp')
- output 8: bfloat16 [8192, 2048], P('tp', 'fsdp')
All inputs are finite; a program needn't handle non-finite values.
Results may differ from the reference program's by a relative error of at most 0.0172669.
Values are sent between devices in bfloat16 or wider.
A program may use at most 1 GiB of HBM per device.

```python
import math
import jax
import jax.numpy as jnp
from jax import lax

BATCH_SIZE = 16
SEQ_LEN = 1024
D_MODEL = 2048
N_HEADS = 8
HEAD_DIM = 256
FF_DIM = 8192
LN_EPS = 1e-6
ROPE_BASE = 10000.0
K_SCALE = 2.5
MASK_VALUE = -1e30


def setup_inputs(seed: int = 0) -> dict:
    rng_keys = jax.random.split(jax.random.key(seed), 8)
    q_cols = N_HEADS * HEAD_DIM
    d_scale = D_MODEL ** -0.5
    kv_scale = jnp.concatenate([jnp.full((HEAD_DIM,), K_SCALE * d_scale, jnp.float32), jnp.full((HEAD_DIM,), d_scale, jnp.float32)])
    x_in = jax.random.normal(rng_keys[0], (BATCH_SIZE, SEQ_LEN, D_MODEL), jnp.float32)
    ln_gain = 1.0 + 0.3 * jax.random.normal(rng_keys[1], (D_MODEL,), jnp.float32)
    w_q = jax.random.normal(rng_keys[2], (D_MODEL, q_cols), jnp.float32) * d_scale
    w_kv = jax.random.normal(rng_keys[3], (D_MODEL, 2 * HEAD_DIM), jnp.float32) * kv_scale
    w_gu = jax.random.normal(rng_keys[4], (D_MODEL, 2, FF_DIM), jnp.float32) * d_scale
    w_oa = jax.random.normal(rng_keys[5], (q_cols, D_MODEL), jnp.float32) * q_cols ** -0.5
    w_om = jax.random.normal(rng_keys[6], (FF_DIM, D_MODEL), jnp.float32) * FF_DIM ** -0.5
    dy_in = jax.random.normal(rng_keys[7], (BATCH_SIZE, SEQ_LEN, D_MODEL), jnp.float32)
    return dict(x_in=x_in.astype(jnp.bfloat16), ln_gain=ln_gain, w_q=w_q.astype(jnp.bfloat16), w_kv=w_kv.astype(jnp.bfloat16), w_gu=w_gu.astype(jnp.bfloat16), w_oa=w_oa.astype(jnp.bfloat16), w_om=w_om.astype(jnp.bfloat16), dy_in=dy_in.astype(jnp.bfloat16))


def rope_tables(seq_len, head_dim):
    half_dim = head_dim // 2
    inv_freq = jnp.exp(jnp.arange(half_dim, dtype=jnp.float32) * (-2.0 * math.log(ROPE_BASE) / head_dim))
    angles = jnp.arange(seq_len, dtype=jnp.float32)[:, None] * inv_freq[None, :]
    return jnp.cos(angles), jnp.sin(angles)


def apply_rope(values, cos_t, sin_t):
    half_dim = values.shape[-1] // 2
    first_half = values[..., :half_dim]
    second_half = values[..., half_dim:]
    return jnp.concatenate([first_half * cos_t - second_half * sin_t, second_half * cos_t + first_half * sin_t], axis=-1)


def layer_norm(x_val, ln_gain):
    x_f32 = x_val.astype(jnp.float32)
    centered = x_f32 - jnp.mean(x_f32, axis=-1, keepdims=True)
    variance = jnp.mean(centered * centered, axis=-1, keepdims=True)
    return (centered * lax.rsqrt(variance + LN_EPS) * ln_gain).astype(jnp.bfloat16)


def layer_row(x_row, ln_gain, w_q, w_kv, w_gu, w_oa, w_om):
    z_row = layer_norm(x_row, ln_gain).astype(jnp.float32)
    q_proj = jnp.dot(z_row, w_q).astype(jnp.bfloat16).reshape(SEQ_LEN, N_HEADS, HEAD_DIM)
    kv_proj = jnp.dot(z_row, w_kv).astype(jnp.bfloat16)
    gu_proj = jnp.dot(z_row, w_gu.reshape(D_MODEL, 2 * FF_DIM)).astype(jnp.bfloat16)
    cos_t, sin_t = rope_tables(SEQ_LEN, HEAD_DIM)
    q_rot = apply_rope(q_proj.astype(jnp.float32), cos_t[:, None, :], sin_t[:, None, :]).astype(jnp.bfloat16).astype(jnp.float32)
    k_rot = apply_rope(kv_proj[:, :HEAD_DIM].astype(jnp.float32), cos_t, sin_t).astype(jnp.bfloat16).astype(jnp.float32)
    v_val = kv_proj[:, HEAD_DIM:].astype(jnp.float32)
    scores = jnp.einsum('qhe,ke->qhk', q_rot, k_rot) * HEAD_DIM ** -0.5
    positions = jnp.arange(SEQ_LEN)
    causal = positions[:, None, None] >= positions[None, None, :]
    scores = jnp.where(causal, scores, MASK_VALUE)
    attn_probs = jax.nn.softmax(scores, axis=-1).astype(jnp.bfloat16).astype(jnp.float32)
    attn_out = jnp.einsum('qhk,ke->qhe', attn_probs, v_val).astype(jnp.bfloat16).reshape(SEQ_LEN, N_HEADS * HEAD_DIM)
    gate_f32 = gu_proj[:, :FF_DIM].astype(jnp.float32)
    up_f32 = gu_proj[:, FF_DIM:].astype(jnp.float32)
    mlp_act = (jax.nn.silu(gate_f32) * up_f32).astype(jnp.bfloat16)
    branch = jnp.dot(attn_out.astype(jnp.float32), w_oa) + jnp.dot(mlp_act.astype(jnp.float32), w_om)
    return (x_row.astype(jnp.float32) + branch).astype(jnp.bfloat16)


def reference(x_in, ln_gain, w_q, w_kv, w_gu, w_oa, w_om, dy_in):
    weights = (w_q.astype(jnp.float32), w_kv.astype(jnp.float32), w_gu.astype(jnp.float32), w_oa.astype(jnp.float32), w_om.astype(jnp.float32))

    def row_step(grad_acc, row_pair):
        x_row, dy_row = row_pair
        y_row, row_vjp = jax.vjp(layer_row, x_row, ln_gain, *weights)
        row_grads = row_vjp(dy_row)
        new_acc = tuple(acc_part + grad_part for acc_part, grad_part in zip(grad_acc, row_grads[1:]))
        return new_acc, (y_row, row_grads[0])

    zero_acc = tuple(jnp.zeros_like(leaf_arr) for leaf_arr in (ln_gain,) + weights)
    grad_sum, (y_out, dx_out) = lax.scan(row_step, zero_acc, (x_in, dy_in))
    return (y_out, dx_out, grad_sum[0], grad_sum[1].astype(jnp.bfloat16), grad_sum[2].astype(jnp.bfloat16), grad_sum[3].astype(jnp.bfloat16), grad_sum[4].astype(jnp.bfloat16), grad_sum[5].astype(jnp.bfloat16))
```

```python
import functools
import math
import jax
import jax.numpy as jnp
from jax import lax
from jax.experimental import pallas as pl
from jax.experimental.pallas import tpu as pltpu
from jax.sharding import PartitionSpec as P

LN_EPS = 1e-6
ROPE_BASE = 10000.0
MASK_VALUE = -1e30
bf16, f32 = jnp.bfloat16, jnp.float32
barrier = lax.optimization_barrier
OUTER = [(0, 1), (1, 0), (2, 3), (3, 2)]
INNER = [(1, 2), (2, 1)]
N_CHUNK = 8
N_QUART = 4


def rope_tables(seq_len, head_dim):
    half_dim = head_dim // 2
    inv_freq = jnp.exp(jnp.arange(half_dim, dtype=f32) * (-2.0 * math.log(ROPE_BASE) / head_dim))
    angles = jnp.arange(seq_len, dtype=f32)[:, None] * inv_freq[None, :]
    return jnp.cos(angles), jnp.sin(angles)


def attn_kernel(heads, blk, qkv_ref, do_ref, cos_ref, sin_ref, o_ref, dqkv_ref, k_s, dk_s, dv_s):
    seq = qkv_ref.shape[0]
    hd = k_s.shape[1]
    half = hd // 2
    nq = heads * hd
    scale = hd ** -0.5

    def rope(a, cos_t, sin_t):
        a = a.astype(f32)
        lo, hi = a[:, :half], a[:, half:]
        return jnp.concatenate([lo * cos_t - hi * sin_t, hi * cos_t + lo * sin_t], axis=1).astype(bf16)

    def unrope(a, cos_t, sin_t):
        lo, hi = a[:, :half], a[:, half:]
        return jnp.concatenate([lo * cos_t + hi * sin_t, hi * cos_t - lo * sin_t], axis=1).astype(bf16)

    k_s[...] = rope(qkv_ref[:, nq:nq + hd], cos_ref[...], sin_ref[...])
    dk_s[...] = jnp.zeros_like(dk_s)
    dv_s[...] = jnp.zeros_like(dv_s)
    tri = lax.broadcasted_iota(jnp.int32, (blk, blk), 0) >= lax.broadcasted_iota(jnp.int32, (blk, blk), 1)
    for i in range(seq // blk):
        r0, kl = i * blk, (i + 1) * blk
        for h in range(heads):
            q = rope(qkv_ref[r0:kl, h * hd:(h + 1) * hd], cos_ref[r0:kl, :], sin_ref[r0:kl, :])
            do = do_ref[r0:kl, h * hd:(h + 1) * hd]
            k, v = k_s[:kl, :], qkv_ref[:kl, nq + hd:nq + 2 * hd]
            s = dot(q, k, NT) * scale
            diag = jnp.where(tri, s[:, r0:], MASK_VALUE)
            s = diag if i == 0 else jnp.concatenate([s[:, :r0], diag], axis=1)
            e = jnp.exp(s - jnp.max(s, axis=1, keepdims=True))
            p = e / jnp.sum(e, axis=1, keepdims=True)
            pb = p.astype(bf16)
            o_ref[r0:kl, h * hd:(h + 1) * hd] = dot(pb, v, NN).astype(bf16)
            dp = dot(do, v, NT)
            ds = (p * (dp - jnp.sum(p * dp, axis=1, keepdims=True)) * scale).astype(bf16)
            dqkv_ref[r0:kl, h * hd:(h + 1) * hd] = unrope(dot(ds, k, NN), cos_ref[r0:kl, :], sin_ref[r0:kl, :])
            dk_s[:kl, :] += dot(ds, q, TN)
            dv_s[:kl, :] += dot(pb, do, TN)
    dqkv_ref[:, nq:nq + hd] = unrope(dk_s[...], cos_ref[...], sin_ref[...])
    dqkv_ref[:, nq + hd:] = dv_s[...].astype(bf16)


def attention(qkv, d_attn, batch, heads):
    rows, width = qkv.shape
    seq, nq = rows // batch, d_attn.shape[1]
    hd = nq // heads
    cos_t, sin_t = rope_tables(seq, hd)
    row = lambda w: pl.BlockSpec((seq, w), lambda b: (b, 0))
    fixed = pl.BlockSpec((seq, hd // 2), lambda b: (0, 0))
    return pl.pallas_call(
        functools.partial(attn_kernel, heads, min(256, seq)),
        grid=(batch,),
        in_specs=[row(width), row(nq), fixed, fixed],
        out_specs=[row(nq), row(width)],
        out_shape=[jax.ShapeDtypeStruct((rows, nq), bf16), jax.ShapeDtypeStruct((rows, width), bf16)],
        scratch_shapes=[pltpu.VMEM((seq, hd), bf16), pltpu.VMEM((seq, hd), f32), pltpu.VMEM((seq, hd), f32)],
        compiler_params=pltpu.CompilerParams(vmem_limit_bytes=56 << 20),
        cost_estimate=pl.CostEstimate(flops=7 * batch * heads * seq * seq * hd, bytes_accessed=rows * width * 6, transcendentals=batch * heads * seq * seq // 2),
        name='attn',
    )(qkv, d_attn, cos_t, sin_t)


def nt_kernel(n_seg, norm, *refs):
    a_refs, w_refs, rest = refs[:n_seg], refs[n_seg:2 * n_seg], refs[2 * n_seg:]
    part = None
    for a_ref, w_ref in zip(a_refs, w_refs):
        term = dot(a_ref[...].reshape(a_ref.shape[-2:]), w_ref[...], NT)
        part = term if part is None else part + term
    if not norm:
        rest[0][...] = part.astype(bf16)
        return
    x_ref, gain_ref, p_ref, dgain_ref, acc = rest
    n = pl.program_id(0)
    nb = part.shape[1]
    acc[:, pl.ds(pl.multiple_of(n * nb, nb), nb)] = part

    @pl.when(n == pl.num_programs(0) - 1)
    def _():
        dgain_ref[...] = jnp.zeros_like(dgain_ref)
        rb = 32

        @pl.loop(0, acc.shape[0] // rb)
        def _(i):
            r = pl.ds(pl.multiple_of(i * rb, rb), rb)
            x = x_ref[r, :].astype(f32)
            mean, rstd = norm_stats(x)
            hat = (x - mean) * rstd
            d_z = acc[r, :]
            g = d_z * gain_ref[...]
            out = g - jnp.mean(g, axis=-1, keepdims=True) - hat * jnp.mean(g * hat, axis=-1, keepdims=True)
            p_ref[r, :] = (rstd * out).astype(bf16)
            dg = d_z * hat
            dgain_ref[...] += dg[:16] + dg[16:]


def nt_sum(j, rows, segs, norm=None):
    a_specs, w_specs, flops = [], [], 0
    d, nb = segs[0][2].shape[0], 512
    for a, plane, w, col in segs:
        depth = a.shape[-1]
        flops += 2 * rows * depth * d
        if plane is None:
            a_specs.append(pl.BlockSpec((rows, depth), lambda n: (j, 0), pipeline_mode=pl.Buffered(1)))
        else:
            a_specs.append(pl.BlockSpec((1, rows, depth), lambda n, plane=plane: (plane, j, 0), pipeline_mode=pl.Buffered(1)))
        w_specs.append(pl.BlockSpec((nb, depth), lambda n, c=col: (n, c)))
    out = pl.BlockSpec((rows, nb), lambda n: (0, n))
    shape = jax.ShapeDtypeStruct((rows, d), bf16)
    specs, ops, scratch = a_specs + w_specs, [s[0] for s in segs] + [s[2] for s in segs], []
    if norm is not None:
        specs += [pl.BlockSpec((rows, d), lambda n: (j, 0), pipeline_mode=pl.Buffered(1)), pl.BlockSpec((1, d), lambda n: (0, 0))]
        ops += list(norm)
        out = [pl.BlockSpec((rows, d), lambda n: (0, 0)), pl.BlockSpec((16, d), lambda n: (0, 0))]
        shape = [shape, jax.ShapeDtypeStruct((16, d), f32)]
        scratch = [pltpu.VMEM((rows, d), f32)]
    return pl.pallas_call(
        functools.partial(nt_kernel, len(segs), norm is not None),
        grid=(d // nb,), in_specs=specs, out_specs=out, out_shape=shape, scratch_shapes=scratch,
        compiler_params=pltpu.CompilerParams(vmem_limit_bytes=58 << 20),
        cost_estimate=pl.CostEstimate(flops=flops, bytes_accessed=flops // 400, transcendentals=0),
        name='dz' if norm is not None else 'y',
    )(*ops)


def dm_kernel(dy_ref, w_ref, g_ref, u_ref, *rest):
    o_ref = rest[-1]
    nb = 256
    for n in range(w_ref.shape[1] // nb):
        c = slice(n * nb, (n + 1) * nb)
        d_m = dot(dy_ref[...], w_ref[:, c], NN).astype(bf16).astype(f32)
        g, u = g_ref[:, c].astype(f32), u_ref[:, c].astype(f32)
        sig = jax.nn.sigmoid(g)
        act = g * sig
        o_ref[0, :, c] = (d_m * u * (sig + act * (1.0 - sig))).astype(bf16)
        o_ref[1, :, c] = (d_m * act).astype(bf16)


def mlp_back(dy2, w_omt, gu_all, half, prev=None):
    rows, d = dy2.shape
    ff = w_omt.shape[1]
    rb, fb = 512, 1024
    nr = rows // rb // 2
    r0 = half * nr
    specs = [pl.BlockSpec((rb, d), lambda f, r: (r0 + r, 0)), pl.BlockSpec((d, fb), lambda f, r: (0, f)),
             pl.BlockSpec((rb, fb), lambda f, r: (r0 + r, f)), pl.BlockSpec((rb, fb), lambda f, r: (r0 + r, ff // fb + f))]
    ops = [dy2, w_omt, gu_all, gu_all]
    if prev is not None:
        specs.append(pl.BlockSpec(memory_space=pl.ANY))
        ops.append(prev)
    return pl.pallas_call(
        dm_kernel, grid=(ff // fb, nr), in_specs=specs,
        out_specs=pl.BlockSpec((2, rb, fb), lambda f, r: (0, r0 + r, f)),
        out_shape=jax.ShapeDtypeStruct((2, rows, ff), bf16),
        input_output_aliases={} if prev is None else {4: 0},
        compiler_params=pltpu.CompilerParams(vmem_limit_bytes=56 << 20),
        cost_estimate=pl.CostEstimate(flops=rows * d * ff, bytes_accessed=5 * rows * ff, transcendentals=rows * ff // 2),
        name='dm',
    )(*ops)


def norm_stats(x_f32):
    mean = jnp.mean(x_f32, axis=-1, keepdims=True)
    centered = x_f32 - mean
    rstd = lax.rsqrt(jnp.mean(centered * centered, axis=-1, keepdims=True) + LN_EPS)
    return mean, rstd


def dot(a, b, dims):
    return lax.dot_general(a, b, (dims, ((), ())), preferred_element_type=f32)


NN = ((1,), (0,))
NT = ((1,), (1,))
TN = ((0,), (0,))


def local_layer(x_in, ln_gain, w_q, w_kv, w_gu, w_oa, w_om, dy_in):
    batch_loc, seq_len, d_model = x_in.shape
    rows = batch_loc * seq_len
    head_dim = w_kv.shape[1] // 2
    nq, nkv, ff = w_q.shape[1], w_kv.shape[1], w_om.shape[0]
    heads = nq // head_dim
    cr, qr = rows // N_CHUNK, rows // N_QUART
    per_q = N_CHUNK // N_QUART

    local_a = jnp.concatenate([w_q, w_kv, w_oa.T], axis=1)
    wa = lax.all_gather(local_a, 'fsdp', axis=0, tiled=True)
    local_b, local_c, _ = barrier((w_gu.reshape(w_gu.shape[0], 2 * ff), w_om.T, local_a))
    w_gum = lax.all_gather(local_b, 'fsdp', axis=0, tiled=True)
    w_omt = lax.all_gather(local_c, 'fsdp', axis=0, tiled=True)
    w_qkv, w_oat = wa[:, :nq + nkv], wa[:, nq + nkv:]

    x2 = x_in.reshape(rows, d_model)
    dy2 = dy_in.reshape(rows, d_model)
    mean, rstd = norm_stats(x2.astype(f32))
    z_act = ((x2.astype(f32) - mean) * rstd * ln_gain).astype(bf16)

    qkv = dot(z_act, w_qkv, NN).astype(bf16)
    d_attn = dot(dy2, w_oat, NN).astype(bf16)
    attn, d_qkv = attention(qkv, d_attn, batch_loc, heads)
    dwa = jnp.concatenate([dot(z_act, d_qkv, TN).astype(bf16), dot(dy2, attn, TN).astype(bf16)], axis=1)
    attn, d_qkv, dwa, w_gum = barrier((attn, d_qkv, dwa, w_gum))

    def rowblock(a, j):
        return a[j * qr:(j + 1) * qr]

    val = {'dwa': dwa}

    gu_all = dot(z_act, w_gum, NN).astype(bf16)
    m_all = (jax.nn.silu(gu_all[:, :ff].astype(f32)) * gu_all[:, ff:].astype(f32)).astype(bf16)
    gu_all, m_all, w_omt = barrier((gu_all, m_all, w_omt))

    def y_block(j, gate):
        val['p', j] = nt_sum(j, qr, [(gate(attn), None, wa, (nq + nkv) // nq), (m_all, None, w_omt, 0)])
        return [('p', j)]

    def dm_block(half, gate):
        val['dgu'] = mlp_back(gate(dy2), w_omt, gu_all, half, val.get('dgu'))
        return ['dgu']

    def dz_block(j, gate):
        segs = [(gate(d_qkv), None, wa, 0), (val['dgu'], 0, w_gum, 0), (val['dgu'], 1, w_gum, 1)]
        val['p', N_QUART + j], val['gain', j] = nt_sum(j, qr, segs, (x2, ln_gain[None]))
        return [('p', N_QUART + j), ('gain', j)]

    def dwom_block(gate):
        val['dwom'] = dot(gate(dy2), m_all, TN).astype(bf16)
        return ['dwom']

    def dwg_block(gate):
        val['dwg'] = dot(gate(z_act), val['dgu'][0], TN).astype(bf16)
        return ['dwg']

    def dwu_block(gate):
        val['dwu'] = dot(gate(z_act), val['dgu'][1], TN).astype(bf16)
        return ['dwu']

    def scatter(out, src, gate):
        val[out] = lax.psum_scatter(val[src], 'fsdp', scatter_dimension=0, tiled=True)
        return []

    def kv_sum(gate):
        val['dw_kv'] = lax.psum(val['rs_a'][:, nq:nq + nkv], 'tp')
        return []

    def gain_sum(gate):
        part = jnp.sum(sum(gate(val['gain', j]) for j in range(N_QUART)), axis=0)
        val['gain'] = lax.psum(part, 'fsdp')
        return ['gain']

    def gain_hop(step, gate):
        if step == 0:
            val['g_in'] = lax.ppermute(gate(val['gain']), 'tp', OUTER)
            return ['g_in']
        if step == 1:
            val['gain'] = gate(val['gain']) + val['g_in']
            val['g_in'] = lax.ppermute(val['gain'], 'tp', INNER)
            return ['gain', 'g_in']
        val['gain'] = gate(val['gain']) + val['g_in']
        val['g_in'] = lax.ppermute(val['gain'], 'tp', OUTER)
        return ['gain', 'g_in']

    def due(key, gate):
        return [key]

    if N_CHUNK == 8:
        plan = {
            0: [('scatter', 'rs_a', 'dwa'), ('y', 1)], 1: [('y', 2)], 2: [('y', 3)],
            3: [('due', 'rs_a'), ('dm', 0)], 4: [('kv',), ('dm', 1)], 5: [('dz', 0)], 6: [('dwom',), ('due', 'dw_kv')],
            7: [('scatter', 'rs_om', 'dwom'), ('dz', 1)], 8: [('dwg',)],
            9: [('dz', 2), ('scatter', 'rs_g', 'dwg')], 10: [('dwu',)], 11: [('dz', 3), ('scatter', 'rs_u', 'dwu'), ('due', 'rs_om')],
            12: [('gain',)], 13: [('hop', 0)], 14: [('hop', 1), ('due', 'rs_g')], 15: [('hop', 2)], 17: [('due', 'rs_u')],
        }
    else:
        plan = {
            0: [('scatter', 'rs_a', 'dwa'), ('y', 1), ('dm', 0)], 1: [('y', 2), ('dm', 1)],
            2: [('y', 3), ('due', 'rs_a'), ('dwom',)], 3: [('scatter', 'rs_om', 'dwom'), ('kv',), ('dz', 0)], 4: [('dwg',), ('dz', 1), ('due', 'dw_kv')],
            5: [('scatter', 'rs_g', 'dwg'), ('dwu',), ('dz', 2)], 6: [('scatter', 'rs_u', 'dwu'), ('due', 'rs_om'), ('dz', 3)],
            7: [('gain',), ('hop', 0), ('due', 'rs_g')], 8: [('hop', 1)], 9: [('hop', 2), ('due', 'rs_u')],
        }
    blocks = dict(y=y_block, dm=dm_block, dz=dz_block, dwom=dwom_block, dwg=dwg_block, dwu=dwu_block,
                  scatter=scatter, kv=kv_sum, gain=gain_sum, hop=gain_hop, due=due)

    y_block(0, lambda a: a)

    z_idx = lax.axis_index('tp')
    at_end = (z_idx == 0) | (z_idx == 3)
    total = 2 * N_CHUNK

    def part(k):
        blk = val['p', k // per_q]
        o = (k % per_q) * cr
        return blk[o:o + cr]

    got1, got2, sum1, sent = {}, {}, {}, {}
    outs = [jnp.zeros((rows, d_model), bf16), jnp.zeros((rows, d_model), bf16)]
    bases = [x2, dy2]

    def finish(k, gate):
        side, o = k // N_CHUNK, (k % N_CHUNK) * cr
        summed = jnp.where(at_end, gate(got1[k + 2]), sent[k + 2])
        new = (bases[side][o:o + cr].astype(f32) + summed.astype(f32)).astype(bf16)
        outs[side] = lax.dynamic_update_slice(outs[side], new, (o, 0))
        val['out', side] = outs[side]
        return [('out', side)]

    for t in range(total + 2):
        tot = sum1[t - 2] + got2[t - 1] if t >= 2 else None
        if t < total:
            pay1 = part(t) if tot is None else jnp.where(at_end, part(t), tot)
        else:
            pay1 = tot
        pay2 = None
        if 1 <= t <= total:
            pay2 = part(t - 1) + got1[t - 1]
        if pay2 is None:
            pay1 = barrier(pay1)
        else:
            pay1, pay2 = barrier((pay1, pay2))
            sum1[t - 1] = pay2
        sent[t] = pay1
        got1[t] = lax.ppermute(pay1, 'tp', OUTER)
        if pay2 is not None:
            got2[t] = lax.ppermute(pay2, 'tp', INNER)
        gate = lambda a: barrier((a, pay1))[0]
        keys = []
        for unit in plan.get(t, []):
            keys += blocks[unit[0]](*unit[1:], gate)
        if t >= 3:
            keys += finish(t - 3, gate)
        perms = [got1[t]] + ([got2[t]] if pay2 is not None else [])
        held = barrier(tuple(perms + [val[k] for k in keys]))
        got1[t] = held[0]
        if pay2 is not None:
            got2[t] = held[1]
        for k, v in zip(keys, held[len(perms):]):
            val[k] = v
            if k[0] == 'out':
                outs[k[1]] = v
    finish(total - 1, lambda a: a)

    rs_a, dw_kv = val['rs_a'], val['dw_kv']
    gain = jnp.where(at_end, val['g_in'], val['gain'])
    dw_gu = jnp.stack([val['rs_g'], val['rs_u']], axis=1)
    y_out, dx_out = outs[0].reshape(x_in.shape), outs[1].reshape(x_in.shape)
    return (y_out, dx_out, gain, rs_a[:, :nq], dw_kv, dw_gu, rs_a[:, nq + nkv:].T, val['rs_om'].T)


def solution(mesh):
    return jax.shard_map(
        local_layer, mesh=mesh,
        in_specs=(P('fsdp'), P(), P('fsdp', 'tp'), P('fsdp', None), P('fsdp', None, 'tp'), P('tp', 'fsdp'), P('tp', 'fsdp'), P('fsdp')),
        out_specs=(P('fsdp'), P('fsdp'), P(), P('fsdp', 'tp'), P('fsdp', None), P('fsdp', None, 'tp'), P('tp', 'fsdp'), P('tp', 'fsdp')),
        check_vma=False)
```
